32 devices in a mesh: ctx: 8 (over z, x), head: 4 (over y, core).
Axes of the slice: x: 2, y: 2, z: 4, core: 2. Of those that a mesh axis runs over, the one named last changes fastest.
Arguments:
- queries: bfloat16 [2048, 2048], P(('ctx', 'head')), may hold values from -6 to 6
- key_vectors_state: bfloat16 [2048, 512], P(('ctx', 'head')), may hold values from -6 to 6
- value_vectors_state: bfloat16 [2048, 512], P(('ctx', 'head')), may hold values from -6 to 6
- doc_bounds: int32 [17], replicated, may hold values from 0 to 2048, as said below
Outputs:
- attended: bfloat16 [2048, 2048], P(('ctx', 'head'))
The draws below stay inside these ranges and needn't reach their ends.
Inputs may be any that keep to these rules, and one draw needn't show every extreme that they name: doc_bounds[0] is 0 and doc_bounds[16] is 2048; the entries strictly increase, and doc_bounds[1] to doc_bounds[15] all lie below 1024, so the last document holds at least half of the tokens.
All inputs are finite; a program needn't handle non-finite values.
Results may differ from the reference program's by a relative error of at most 0.004.
Values may be sent and summed in bfloat16 or wider, within the bound.
A program may use at most 64 MiB of HBM per device.

```python
import math
import jax
import jax.numpy as jnp
from jax import lax

QUERY_HEADS = 32
KEY_VALUE_HEADS = 8
HEAD_SIZE = 64
DOCS = 16
PACKED_TOKENS = 2048


def draw_queries(key, part):
    base_value = jax.random.fold_in(key, 21)
    drawn_sample = jnp.clip(jax.random.normal(base_value, (PACKED_TOKENS, QUERY_HEADS * HEAD_SIZE), jnp.float32), -6.0, 6.0)
    return drawn_sample.astype(jnp.bfloat16)


def draw_key_vectors_state(key, part):
    base_value = jax.random.fold_in(key, 22)
    drawn_sample = jnp.clip(jax.random.normal(base_value, (PACKED_TOKENS, KEY_VALUE_HEADS * HEAD_SIZE), jnp.float32), -6.0, 6.0)
    return drawn_sample.astype(jnp.bfloat16)


def draw_doc_bounds(key, part):
    cuts = jax.random.permutation(jax.random.fold_in(key, 31), PACKED_TOKENS // 2 - 1)[:DOCS - 1] + 1
    cuts = jnp.sort(cuts.astype(jnp.int32))
    return jnp.concatenate([jnp.zeros((1,), jnp.int32), cuts, jnp.full((1,), PACKED_TOKENS, jnp.int32)])


def block_levels(own_key, dims, split, low, high):
    def one(position, shards_of):
        draws = jax.random.uniform(jax.random.fold_in(jax.random.fold_in(own_key, 6), position), (shards_of,), jnp.float32, low / len(split), high / len(split))
        return jnp.repeat(jnp.exp(draws), dims[position] // shards_of).reshape((-1,) + (1,) * (len(dims) - position - 1))

    factor_of = one(*split[0])
    for cut in split[1:]:
        factor_of = factor_of * one(*cut)
    return factor_of


def centred(rng, dims, deviation, reach, shards=(), held_as=jnp.bfloat16):
    drawn = deviation * jax.random.normal(rng, dims, jnp.float32)
    if shards:
        drawn = drawn * block_levels(rng, dims, shards, -0.22, 0.18)
    return jnp.clip(drawn, -reach, reach).astype(held_as)


def setup_inputs(seed: int = 0) -> dict:
    streams_of = jax.random.split(jax.random.key(seed), 5)
    return {
        "queries": draw_queries(jax.random.fold_in(streams_of[4], 71), 0),
        "key_vectors_state": draw_key_vectors_state(jax.random.fold_in(streams_of[4], 71), 0),
        "value_vectors_state": centred(streams_of[2], (PACKED_TOKENS, KEY_VALUE_HEADS * HEAD_SIZE), 1.0, 6.0, ((0, 32),)),
        "doc_bounds": draw_doc_bounds(jax.random.fold_in(streams_of[4], 71), 0),
    }


masked_score = -1e+30

def document_of(positions, doc_bounds):
    interior = doc_bounds[1:-1]
    return lax.optimization_barrier(jnp.sum((interior[None, :] <= positions[:, None]).astype(jnp.int32), axis=1))

def reference(queries, key_vectors_state, value_vectors_state, doc_bounds):
    sequence_length = queries.shape[0]
    queries_per_group = QUERY_HEADS // KEY_VALUE_HEADS
    score_scale = 1.0 / math.sqrt(HEAD_SIZE)
    heads_of_queries = queries.reshape(sequence_length, KEY_VALUE_HEADS, queries_per_group, HEAD_SIZE)
    heads_of_keys = key_vectors_state.reshape(sequence_length, KEY_VALUE_HEADS, HEAD_SIZE)
    heads_of_values = value_vectors_state.reshape(sequence_length, KEY_VALUE_HEADS, HEAD_SIZE)
    positions = jnp.arange(sequence_length, dtype=jnp.int32)
    doc_ids = document_of(positions, doc_bounds)
    row_block = min(512, sequence_length)
    num_blocks = sequence_length // row_block

    def one_block(block_index):
        anchor = (block_index * row_block).astype(jnp.int32)
        query_block = lax.dynamic_slice_in_dim(heads_of_queries, anchor, row_block, 0)
        query_pos = anchor + jnp.arange(row_block, dtype=jnp.int32)
        query_doc = lax.dynamic_slice_in_dim(doc_ids, anchor, row_block, 0)
        allowed = (query_doc[:, None] == doc_ids[None, :]) & (positions[None, :] <= query_pos[:, None])
        visible = allowed[:, None, :]

        def single_head(head_index):
            query_group = lax.dynamic_index_in_dim(query_block, head_index, 1, keepdims=False)
            key_group = lax.dynamic_index_in_dim(heads_of_keys, head_index, 1, keepdims=False)
            value_group = lax.dynamic_index_in_dim(heads_of_values, head_index, 1, keepdims=False)
            scores = jnp.einsum('qjd,kd->qjk', query_group.astype(jnp.float32), key_group.astype(jnp.float32)) * score_scale
            masked = jnp.where(visible, scores, masked_score)
            top_score = lax.optimization_barrier(jnp.max(masked, axis=-1))
            weights = jnp.exp(masked - top_score[..., None]) * visible.astype(jnp.float32)
            weight_sum = lax.optimization_barrier(jnp.sum(weights, axis=-1))
            rounded = lax.optimization_barrier(weights.astype(jnp.bfloat16))
            mixed = jnp.einsum('qjk,kd->qjd', rounded.astype(jnp.float32), value_group.astype(jnp.float32))
            return (mixed / weight_sum[..., None]).astype(jnp.bfloat16)
        output_heads = lax.map(single_head, jnp.arange(KEY_VALUE_HEADS, dtype=jnp.int32))
        return jnp.transpose(output_heads, (1, 0, 2, 3))
    blocks_out = lax.map(one_block, jnp.arange(num_blocks, dtype=jnp.int32))
    return blocks_out.reshape(sequence_length, QUERY_HEADS * HEAD_SIZE)
```

```python
import functools
import math

import jax
import jax.numpy as jnp
from jax import lax
from jax.experimental import pallas as pl
from jax.experimental.pallas import tpu as pltpu
from jax.sharding import PartitionSpec as P

HEAD_SIZE = 64
LANES = 128
MESH = pl.DeviceIdType.MESH

masked_score = -1e30
exp2_scale = math.log2(math.e) / math.sqrt(HEAD_SIZE)


def kernel(
    n_ctx, n_head, members, reach_start,
    bounds_ref, q_hbm, k_hbm, v_hbm, out_ref,
    q_in, k_in, v_in, kv_own, q_buf, kv_buf, key_even, key_odd, value_even, value_odd,
    doc_start, bias, top, acc, o_buf,
    in_sem, kv_send, q_send, slab_send, o_send, kv_recv, q_recv, o_recv,
):
    rows = q_in.shape[0]
    group_cols = q_in.shape[1] // members
    tiles = group_cols // LANES
    slab = rows * members
    half = slab // 2
    span = members // n_head
    planes = n_ctx // span
    my_ctx, my_head = lax.axis_index("ctx"), lax.axis_index("head")
    plane = my_ctx // span
    member = lax.rem(my_ctx, span) * n_head + my_head
    reach_slab, reach_row = reach_start // slab, reach_start % slab

    def at(plane_index, member_index):
        return (plane_index * span + member_index // n_head, lax.rem(member_index, n_head))

    def partner(turn):
        return lax.rem(member + turn, members)

    loads = [
        pltpu.make_async_copy(k_hbm, k_in, in_sem.at[0]),
        pltpu.make_async_copy(v_hbm, v_in, in_sem.at[1]),
        pltpu.make_async_copy(q_hbm, q_in, in_sem.at[2]),
    ]
    for load in loads:
        load.start()

    barrier = pltpu.get_barrier_semaphore()
    for turn in range(1, members):
        pl.semaphore_signal(barrier, inc=1, device_id=at(plane, partner(turn)), device_id_type=MESH)
    for step in range(1, planes):
        other = lax.rem(plane + step, planes)
        pl.semaphore_signal(barrier, inc=1, device_id=at(other, member), device_id_type=MESH)

    def low_lanes(count):
        return lax.broadcasted_iota(jnp.int32, (count, LANES), 1) < HEAD_SIZE

    loads[0].wait()
    loads[1].wait()
    low = low_lanes(rows)
    for pair in range(members // 2):
        columns = slice(pair * LANES, (pair + 1) * LANES)
        keys = k_in[:, columns].astype(jnp.float32)
        values = v_in[:, columns].astype(jnp.float32)
        kv_own[2 * pair] = jnp.where(low, keys, pltpu.roll(values, HEAD_SIZE, 1)).astype(jnp.bfloat16)
        kv_own[2 * pair + 1] = jnp.where(low, pltpu.roll(keys, HEAD_SIZE, 1), values).astype(jnp.bfloat16)
    loads[2].wait()

    pl.semaphore_wait(barrier, members - 1 + planes - 1)

    my_rows = pl.ds(pl.multiple_of(member * rows, rows), rows)
    kv_copies, q_copies = [], []
    for turn in range(1, members):
        to = partner(turn)
        copy = pltpu.make_async_remote_copy(
            src_ref=kv_own.at[to],
            dst_ref=kv_buf.at[plane, my_rows],
            send_sem=kv_send.at[turn - 1],
            recv_sem=kv_recv.at[plane],
            device_id=at(plane, to),
            device_id_type=MESH,
        )
        copy.start()
        kv_copies.append(copy)
    pltpu.make_async_copy(kv_own.at[member], kv_buf.at[plane, my_rows], kv_recv.at[plane]).start()
    for turn in range(1, members):
        to = partner(turn)
        copy = pltpu.make_async_remote_copy(
            src_ref=q_in.at[:, pl.ds(pl.multiple_of(to * group_cols, LANES), group_cols)],
            dst_ref=q_buf.at[my_rows],
            send_sem=q_send.at[turn - 1],
            recv_sem=q_recv,
            device_id=at(plane, to),
            device_id_type=MESH,
        )
        copy.start()
        q_copies.append(copy)
    pltpu.make_async_copy(
        q_in.at[:, pl.ds(pl.multiple_of(member * group_cols, LANES), group_cols)],
        q_buf.at[my_rows],
        q_recv,
    ).start()

    position = plane * slab + lax.broadcasted_iota(jnp.int32, (slab, LANES), 0)
    start = jnp.zeros((slab, LANES), jnp.int32)
    for doc in range(1, bounds_ref.shape[0] - 1):
        bound = bounds_ref[doc]
        start = jnp.where(position >= bound, bound, start)
    doc_start[...] = start

    def fill_bias(first_key, count, causal):
        for block in range(2):
            here = slice(block * half, (block + 1) * half)
            key = first_key + lax.broadcasted_iota(jnp.int32, (half, count), 1)
            allowed = key >= jnp.tile(doc_start[here], (1, count // LANES))
            if causal:
                query = plane * slab + block * half + lax.broadcasted_iota(jnp.int32, (half, count), 0)
                allowed = allowed & (key <= query)
            bias[here, :count] = jnp.where(allowed, 0.0, masked_score)

    fill_bias(plane * slab, slab, True)

    pltpu.make_async_copy(kv_buf.at[plane], kv_buf.at[plane], kv_recv.at[plane]).wait()

    def slab_copy(step, first_row):
        piece = kv_buf.at[plane] if first_row == 0 else kv_buf.at[plane, pl.ds(first_row, slab - first_row)]
        return pltpu.make_async_remote_copy(
            src_ref=piece,
            dst_ref=piece,
            send_sem=slab_send.at[step - 1],
            recv_sem=kv_recv.at[plane],
            device_id=at(plane + step, member),
            device_id_type=MESH,
        )

    def each_slab_copy(act):
        for step in range(1, planes):
            to = plane + step
            if reach_start == 0:
                pl.when(to < planes)(lambda: act(slab_copy(step, 0)))
            else:
                early = to < planes // 2
                later = plane > reach_slab if reach_row else plane >= reach_slab
                pl.when((to < planes) & (early | later))(lambda: act(slab_copy(step, 0)))
                if reach_row:
                    part = (to < planes) & (to >= planes // 2) & (plane == reach_slab)
                    pl.when(part)(lambda: act(slab_copy(step, reach_row)))

    each_slab_copy(lambda copy: copy.start())

    def spread(source, first_row):
        count = slab - first_row
        low = low_lanes(count)
        kv = kv_buf[source, first_row:].astype(jnp.float32)
        swapped = pltpu.roll(kv, HEAD_SIZE, 1)
        key_even[:count] = jnp.where(low, kv, 0.0).astype(jnp.bfloat16)
        key_odd[:count] = jnp.where(low, 0.0, swapped).astype(jnp.bfloat16)
        value_even[:count] = jnp.where(low, swapped, 1.0).astype(jnp.bfloat16)
        value_odd[:count] = jnp.where(low, 1.0, kv).astype(jnp.bfloat16)

    def attend(tile, block, count, opening):
        here = slice(block * half, (block + 1) * half)
        queries = q_buf[here, pl.ds(pl.multiple_of(tile * LANES, LANES), LANES)]
        for parity, (key, value) in enumerate(((key_even, value_even), (key_odd, value_odd))):
            scores = lax.dot_general(
                queries, key[:count], (((1,), (1,)), ((), ())), preferred_element_type=jnp.float32
            ) + bias[here, :count]
            peak = jnp.max(scores, axis=1, keepdims=True)
            if opening:
                new_top = jnp.broadcast_to(peak, (half, LANES))
            else:
                old_top = top[tile, parity, here]
                new_top = jnp.maximum(old_top, peak)
            weights = jnp.exp2((scores - jnp.tile(new_top, (1, count // LANES))) * exp2_scale)
            mixed = jnp.dot(
                weights.astype(jnp.bfloat16), value[:count], preferred_element_type=jnp.float32
            )
            if not opening:
                mixed = mixed + acc[tile, parity, here] * jnp.exp2((old_top - new_top) * exp2_scale)
            top[tile, parity, here] = new_top
            acc[tile, parity, here] = mixed

    spread(plane, 0)
    pltpu.make_async_copy(q_buf, q_buf, q_recv).wait()

    @pl.loop(0, tiles)
    def _(tile):
        attend(tile, 0, half, True)
        attend(tile, 1, slab, True)

    def fold(source, first_row):
        piece = kv_buf.at[source] if first_row == 0 else kv_buf.at[source, pl.ds(first_row, slab - first_row)]
        fill_bias(source * slab + first_row, slab - first_row, False)
        pltpu.make_async_copy(piece, piece, kv_recv.at[source]).wait()
        spread(source, first_row)

        @pl.loop(0, tiles)
        def _(tile):
            for block in range(2):
                attend(tile, block, slab - first_row, False)

    if reach_start == 0:
        whole_slabs = plane
    else:
        kept = plane - reach_slab - (1 if reach_row else 0)
        whole_slabs = jnp.where(plane < planes // 2, plane, kept)

    @pl.loop(0, whole_slabs)
    def _(back):
        fold(plane - 1 - back, 0)

    if reach_row:
        pl.when(plane >= planes // 2)(lambda: fold(reach_slab, reach_row))

    low = low_lanes(slab)
    for tile in range(tiles):
        even, odd = acc[tile, 0], acc[tile, 1]
        total = pltpu.roll(jnp.where(low, odd, even), HEAD_SIZE, 1)
        o_buf[:, tile * LANES:(tile + 1) * LANES] = (jnp.where(low, even, odd) / total).astype(jnp.bfloat16)

    my_columns = pl.ds(pl.multiple_of(member * group_cols, LANES), group_cols)
    o_copies = []
    for turn in range(1, members):
        to = partner(turn)
        copy = pltpu.make_async_remote_copy(
            src_ref=o_buf.at[pl.ds(pl.multiple_of(to * rows, rows), rows)],
            dst_ref=out_ref.at[:, my_columns],
            send_sem=o_send.at[turn - 1],
            recv_sem=o_recv,
            device_id=at(plane, to),
            device_id_type=MESH,
        )
        copy.start()
        o_copies.append(copy)
    pltpu.make_async_copy(o_buf.at[my_rows], out_ref.at[:, my_columns], o_recv).start()

    for copy in kv_copies + q_copies:
        copy.wait_send()
    each_slab_copy(lambda copy: copy.wait_send())
    for copy in o_copies:
        copy.wait_send()
    pltpu.make_async_copy(out_ref, out_ref, o_recv).wait()


def exchange(n_ctx, n_head, reach_start, collective_id, queries, keys, values, doc_bounds):
    rows, query_cols = queries.shape
    members = keys.shape[1] // HEAD_SIZE
    group_cols = query_cols // members
    slab = rows * members
    planes = n_ctx * n_head // members
    tiles = group_cols // LANES
    bf16, f32 = jnp.bfloat16, jnp.float32
    dma = pltpu.SemaphoreType.DMA
    return pl.pallas_call(
        functools.partial(kernel, n_ctx, n_head, members, reach_start),
        out_shape=jax.ShapeDtypeStruct((rows, query_cols), bf16),
        in_specs=[pl.BlockSpec(memory_space=pltpu.SMEM)] + [pl.BlockSpec(memory_space=pl.ANY)] * 3,
        out_specs=pl.BlockSpec(memory_space=pl.ANY),
        scratch_shapes=[
            pltpu.VMEM((rows, query_cols), bf16),
            pltpu.VMEM(keys.shape, bf16),
            pltpu.VMEM(values.shape, bf16),
            pltpu.VMEM((members, rows, LANES), bf16),
            pltpu.VMEM((slab, group_cols), bf16),
            pltpu.VMEM((planes, slab, LANES), bf16),
            pltpu.VMEM((slab, LANES), bf16),
            pltpu.VMEM((slab, LANES), bf16),
            pltpu.VMEM((slab, LANES), bf16),
            pltpu.VMEM((slab, LANES), bf16),
            pltpu.VMEM((slab, LANES), jnp.int32),
            pltpu.VMEM((slab, slab), f32),
            pltpu.VMEM((tiles, 2, slab, LANES), f32),
            pltpu.VMEM((tiles, 2, slab, LANES), f32),
            pltpu.VMEM((slab, group_cols), bf16),
            dma((3,)),
            dma((members - 1,)),
            dma((members - 1,)),
            dma((planes - 1,)),
            dma((members - 1,)),
            dma((planes,)),
            dma,
            dma,
        ],
        compiler_params=pltpu.CompilerParams(collective_id=collective_id, has_side_effects=True),
    )(doc_bounds, queries, keys, values)


def solution(mesh):
    n_ctx, n_head = mesh.shape["ctx"], mesh.shape["head"]

    def on_device(queries, keys, values, doc_bounds):
        return exchange(n_ctx, n_head, 0, 0, queries, keys, values, doc_bounds)

    return jax.shard_map(
        on_device,
        mesh=mesh,
        in_specs=(P(("ctx", "head"), None),) * 3 + (P(),),
        out_specs=P(("ctx", "head"), None),
        check_vma=False,
    )
```

```python
import functools
import math

import jax
import jax.numpy as jnp
from jax import lax
from jax.experimental import pallas as pl
from jax.experimental.pallas import tpu as pltpu
from jax.sharding import PartitionSpec as P

HEAD_SIZE = 64
LANES = 128
MESH = pl.DeviceIdType.MESH

masked_score = -1e30
exp2_scale = math.log2(math.e) / math.sqrt(HEAD_SIZE)


def kernel(
    n_ctx, n_head, members, reach_start,
    bounds_ref, q_hbm, k_hbm, v_hbm, out_ref,
    q_in, k_in, v_in, kv_own, q_buf, kv_buf, key_even, key_odd, value_even, value_odd,
    doc_start, bias, top, acc, o_buf,
    in_sem, kv_send, q_send, slab_send, o_send, kv_recv, q_recv, o_recv,
):
    rows = q_in.shape[0]
    group_cols = q_in.shape[1] // members
    tiles = group_cols // LANES
    slab = rows * members
    half = slab // 2
    span = members // n_head
    planes = n_ctx // span
    my_ctx, my_head = lax.axis_index("ctx"), lax.axis_index("head")
    plane = my_ctx // span
    member = lax.rem(my_ctx, span) * n_head + my_head
    reach_slab, reach_row = reach_start // slab, reach_start % slab

    def at(plane_index, member_index):
        return (plane_index * span + member_index // n_head, lax.rem(member_index, n_head))

    def partner(turn):
        return lax.rem(member + turn, members)

    loads = [
        pltpu.make_async_copy(k_hbm, k_in, in_sem.at[0]),
        pltpu.make_async_copy(v_hbm, v_in, in_sem.at[1]),
        pltpu.make_async_copy(q_hbm, q_in, in_sem.at[2]),
    ]
    for load in loads:
        load.start()

    barrier = pltpu.get_barrier_semaphore()
    for turn in range(1, members):
        pl.semaphore_signal(barrier, inc=1, device_id=at(plane, partner(turn)), device_id_type=MESH)
    for step in range(1, planes):
        other = lax.rem(plane + step, planes)
        pl.semaphore_signal(barrier, inc=1, device_id=at(other, member), device_id_type=MESH)

    def low_lanes(count):
        return lax.broadcasted_iota(jnp.int32, (count, LANES), 1) < HEAD_SIZE

    loads[0].wait()
    loads[1].wait()
    low = low_lanes(rows)
    for pair in range(members // 2):
        columns = slice(pair * LANES, (pair + 1) * LANES)
        keys = k_in[:, columns].astype(jnp.float32)
        values = v_in[:, columns].astype(jnp.float32)
        kv_own[2 * pair] = jnp.where(low, keys, pltpu.roll(values, HEAD_SIZE, 1)).astype(jnp.bfloat16)
        kv_own[2 * pair + 1] = jnp.where(low, pltpu.roll(keys, HEAD_SIZE, 1), values).astype(jnp.bfloat16)
    loads[2].wait()

    pl.semaphore_wait(barrier, members - 1 + planes - 1)

    my_rows = pl.ds(pl.multiple_of(member * rows, rows), rows)
    kv_copies, q_copies = [], []
    for turn in range(1, members):
        to = partner(turn)
        copy = pltpu.make_async_remote_copy(
            src_ref=kv_own.at[to],
            dst_ref=kv_buf.at[plane, my_rows],
            send_sem=kv_send.at[turn - 1],
            recv_sem=kv_recv.at[plane],
            device_id=at(plane, to),
            device_id_type=MESH,
        )
        copy.start()
        kv_copies.append(copy)
    pltpu.make_async_copy(kv_own.at[member], kv_buf.at[plane, my_rows], kv_recv.at[plane]).start()
    for turn in range(1, members):
        to = partner(turn)
        copy = pltpu.make_async_remote_copy(
            src_ref=q_in.at[:, pl.ds(pl.multiple_of(to * group_cols, LANES), group_cols)],
            dst_ref=q_buf.at[my_rows],
            send_sem=q_send.at[turn - 1],
            recv_sem=q_recv,
            device_id=at(plane, to),
            device_id_type=MESH,
        )
        copy.start()
        q_copies.append(copy)
    pltpu.make_async_copy(
        q_in.at[:, pl.ds(pl.multiple_of(member * group_cols, LANES), group_cols)],
        q_buf.at[my_rows],
        q_recv,
    ).start()

    position = plane * slab + lax.broadcasted_iota(jnp.int32, (slab, LANES), 0)
    start = jnp.zeros((slab, LANES), jnp.int32)
    for doc in range(1, bounds_ref.shape[0] - 1):
        bound = bounds_ref[doc]
        start = jnp.where(position >= bound, bound, start)
    doc_start[...] = start

    def fill_bias(first_key, count, causal):
        for block in range(2):
            here = slice(block * half, (block + 1) * half)
            key = first_key + lax.broadcasted_iota(jnp.int32, (half, count), 1)
            allowed = key >= jnp.tile(doc_start[here], (1, count // LANES))
            if causal:
                query = plane * slab + block * half + lax.broadcasted_iota(jnp.int32, (half, count), 0)
                allowed = allowed & (key <= query)
            bias[here, :count] = jnp.where(allowed, 0.0, masked_score)

    fill_bias(plane * slab, slab, True)

    pltpu.make_async_copy(kv_buf.at[plane], kv_buf.at[plane], kv_recv.at[plane]).wait()

    def slab_copy(step, first_row):
        piece = kv_buf.at[plane] if first_row == 0 else kv_buf.at[plane, pl.ds(first_row, slab - first_row)]
        return pltpu.make_async_remote_copy(
            src_ref=piece,
            dst_ref=piece,
            send_sem=slab_send.at[step - 1],
            recv_sem=kv_recv.at[plane],
            device_id=at(plane + step, member),
            device_id_type=MESH,
        )

    def each_slab_copy(act):
        for step in range(1, planes):
            to = plane + step
            if reach_start == 0:
                pl.when(to < planes)(lambda: act(slab_copy(step, 0)))
            else:
                early = to < planes // 2
                later = plane > reach_slab if reach_row else plane >= reach_slab
                pl.when((to < planes) & (early | later))(lambda: act(slab_copy(step, 0)))
                if reach_row:
                    part = (to < planes) & (to >= planes // 2) & (plane == reach_slab)
                    pl.when(part)(lambda: act(slab_copy(step, reach_row)))

    each_slab_copy(lambda copy: copy.start())

    def spread(source, first_row):
        count = slab - first_row
        low = low_lanes(count)
        kv = kv_buf[source, first_row:].astype(jnp.float32)
        swapped = pltpu.roll(kv, HEAD_SIZE, 1)
        key_even[:count] = jnp.where(low, kv, 0.0).astype(jnp.bfloat16)
        key_odd[:count] = jnp.where(low, 0.0, swapped).astype(jnp.bfloat16)
        value_even[:count] = jnp.where(low, swapped, 1.0).astype(jnp.bfloat16)
        value_odd[:count] = jnp.where(low, 1.0, kv).astype(jnp.bfloat16)

    def attend(tile, block, count, opening):
        here = slice(block * half, (block + 1) * half)
        queries = q_buf[here, pl.ds(pl.multiple_of(tile * LANES, LANES), LANES)]
        for parity, (key, value) in enumerate(((key_even, value_even), (key_odd, value_odd))):
            scores = lax.dot_general(
                queries, key[:count], (((1,), (1,)), ((), ())), preferred_element_type=jnp.float32
            ) + bias[here, :count]
            peak = jnp.max(scores, axis=1, keepdims=True)
            if opening:
                new_top = jnp.broadcast_to(peak, (half, LANES))
            else:
                old_top = top[tile, parity, here]
                new_top = jnp.maximum(old_top, peak)
            weights = jnp.exp2((scores - jnp.tile(new_top, (1, count // LANES))) * exp2_scale)
            mixed = jnp.dot(
                weights.astype(jnp.bfloat16), value[:count], preferred_element_type=jnp.float32
            )
            if not opening:
                mixed = mixed + acc[tile, parity, here] * jnp.exp2((old_top - new_top) * exp2_scale)
            top[tile, parity, here] = new_top
            acc[tile, parity, here] = mixed

    spread(plane, 0)
    pltpu.make_async_copy(q_buf, q_buf, q_recv).wait()

    @pl.loop(0, tiles)
    def _(tile):
        attend(tile, 0, half, True)
        attend(tile, 1, slab, True)

    def fold(source, first_row):
        piece = kv_buf.at[source] if first_row == 0 else kv_buf.at[source, pl.ds(first_row, slab - first_row)]
        fill_bias(source * slab + first_row, slab - first_row, False)
        pltpu.make_async_copy(piece, piece, kv_recv.at[source]).wait()
        spread(source, first_row)

        @pl.loop(0, tiles)
        def _(tile):
            for block in range(2):
                attend(tile, block, slab - first_row, False)

    if reach_start == 0:
        whole_slabs = plane
    else:
        kept = plane - reach_slab - (1 if reach_row else 0)
        whole_slabs = jnp.where(plane < planes // 2, plane, kept)

    @pl.loop(0, whole_slabs)
    def _(back):
        fold(plane - 1 - back, 0)

    if reach_row:
        pl.when(plane >= planes // 2)(lambda: fold(reach_slab, reach_row))

    low = low_lanes(slab)
    for tile in range(tiles):
        even, odd = acc[tile, 0], acc[tile, 1]
        total = pltpu.roll(jnp.where(low, odd, even), HEAD_SIZE, 1)
        o_buf[:, tile * LANES:(tile + 1) * LANES] = (jnp.where(low, even, odd) / total).astype(jnp.bfloat16)

    my_columns = pl.ds(pl.multiple_of(member * group_cols, LANES), group_cols)
    o_copies = []
    for turn in range(1, members):
        to = partner(turn)
        copy = pltpu.make_async_remote_copy(
            src_ref=o_buf.at[pl.ds(pl.multiple_of(to * rows, rows), rows)],
            dst_ref=out_ref.at[:, my_columns],
            send_sem=o_send.at[turn - 1],
            recv_sem=o_recv,
            device_id=at(plane, to),
            device_id_type=MESH,
        )
        copy.start()
        o_copies.append(copy)
    pltpu.make_async_copy(o_buf.at[my_rows], out_ref.at[:, my_columns], o_recv).start()

    for copy in kv_copies + q_copies:
        copy.wait_send()
    each_slab_copy(lambda copy: copy.wait_send())
    for copy in o_copies:
        copy.wait_send()
    pltpu.make_async_copy(out_ref, out_ref, o_recv).wait()


def exchange(n_ctx, n_head, reach_start, collective_id, queries, keys, values, doc_bounds):
    rows, query_cols = queries.shape
    members = keys.shape[1] // HEAD_SIZE
    group_cols = query_cols // members
    slab = rows * members
    planes = n_ctx * n_head // members
    tiles = group_cols // LANES
    bf16, f32 = jnp.bfloat16, jnp.float32
    dma = pltpu.SemaphoreType.DMA
    return pl.pallas_call(
        functools.partial(kernel, n_ctx, n_head, members, reach_start),
        out_shape=jax.ShapeDtypeStruct((rows, query_cols), bf16),
        in_specs=[pl.BlockSpec(memory_space=pltpu.SMEM)] + [pl.BlockSpec(memory_space=pl.ANY)] * 3,
        out_specs=pl.BlockSpec(memory_space=pl.ANY),
        scratch_shapes=[
            pltpu.VMEM((rows, query_cols), bf16),
            pltpu.VMEM(keys.shape, bf16),
            pltpu.VMEM(values.shape, bf16),
            pltpu.VMEM((members, rows, LANES), bf16),
            pltpu.VMEM((slab, group_cols), bf16),
            pltpu.VMEM((planes, slab, LANES), bf16),
            pltpu.VMEM((slab, LANES), bf16),
            pltpu.VMEM((slab, LANES), bf16),
            pltpu.VMEM((slab, LANES), bf16),
            pltpu.VMEM((slab, LANES), bf16),
            pltpu.VMEM((slab, LANES), jnp.int32),
            pltpu.VMEM((slab, slab), f32),
            pltpu.VMEM((tiles, 2, slab, LANES), f32),
            pltpu.VMEM((tiles, 2, slab, LANES), f32),
            pltpu.VMEM((slab, group_cols), bf16),
            dma((3,)),
            dma((members - 1,)),
            dma((members - 1,)),
            dma((planes - 1,)),
            dma((members - 1,)),
            dma((planes,)),
            dma,
            dma,
        ],
        compiler_params=pltpu.CompilerParams(collective_id=collective_id, has_side_effects=True),
    )(doc_bounds, queries, keys, values)


def solution(mesh):
    n_ctx, n_head = mesh.shape["ctx"], mesh.shape["head"]

    def on_device(queries, keys, values, doc_bounds):
        tokens = n_ctx * n_head * queries.shape[0]
        reach_start = 3 * tokens // 8

        def near(*arrays):
            return exchange(n_ctx, n_head, reach_start, 0, *arrays)

        def far(*arrays):
            return exchange(n_ctx, n_head, 0, 1, *arrays)

        return lax.cond(doc_bounds[-2] >= reach_start, near, far, queries, keys, values, doc_bounds)

    return jax.shard_map(
        on_device,
        mesh=mesh,
        in_specs=(P(("ctx", "head"), None),) * 3 + (P(),),
        out_specs=P(("ctx", "head"), None),
        check_vma=False,
    )
```

```python
import functools
import math

import jax
import jax.numpy as jnp
from jax import lax
from jax.experimental import pallas as pl
from jax.experimental.pallas import tpu as pltpu
from jax.sharding import PartitionSpec as P

HEAD_SIZE = 64
LANES = 128
MESH = pl.DeviceIdType.MESH

masked_score = -1e30
exp2_scale = math.log2(math.e) / math.sqrt(HEAD_SIZE)


def kernel(
    n_ctx, n_head, members, reach_start,
    bounds_ref, q_hbm, k_hbm, v_hbm, out_ref,
    q_in, k_in, v_in, kv_own, q_buf, kv_buf, key_even, key_odd, value_even, value_odd,
    doc_start, bias, top, acc, o_buf,
    in_sem, kv_send, q_send, slab_send, o_send, kv_recv, q_recv, o_recv, ready,
):
    rows = q_in.shape[0]
    group_cols = q_in.shape[1] // members
    tiles = group_cols // LANES
    slab = rows * members
    half = slab // 2
    span = members // n_head
    planes = n_ctx // span
    my_ctx, my_head = lax.axis_index("ctx"), lax.axis_index("head")
    plane = my_ctx // span
    member = lax.rem(my_ctx, span) * n_head + my_head
    reach_slab, reach_row = reach_start // slab, reach_start % slab

    def at(plane_index, member_index):
        return (plane_index * span + member_index // n_head, lax.rem(member_index, n_head))

    def partner(turn):
        return lax.rem(member + turn, members)

    loads = [
        pltpu.make_async_copy(k_hbm, k_in, in_sem.at[0]),
        pltpu.make_async_copy(v_hbm, v_in, in_sem.at[1]),
        pltpu.make_async_copy(q_hbm, q_in, in_sem.at[2]),
    ]
    for load in loads:
        load.start()

    barrier = pltpu.get_barrier_semaphore()
    for turn in range(1, members):
        pl.semaphore_signal(barrier, inc=1, device_id=at(plane, partner(turn)), device_id_type=MESH)
    for step in range(1, planes):
        @pl.when(plane + step < planes)
        def _():
            pl.semaphore_signal(
                barrier, inc=1, device_id=at(plane + step, member), device_id_type=MESH
            )

    def low_lanes(count):
        return lax.broadcasted_iota(jnp.int32, (count, LANES), 1) < HEAD_SIZE

    loads[0].wait()
    loads[1].wait()
    low = low_lanes(rows)
    for pair in range(members // 2):
        columns = slice(pair * LANES, (pair + 1) * LANES)
        keys = k_in[:, columns].astype(jnp.float32)
        values = v_in[:, columns].astype(jnp.float32)
        kv_own[2 * pair] = jnp.where(low, keys, pltpu.roll(values, HEAD_SIZE, 1)).astype(jnp.bfloat16)
        kv_own[2 * pair + 1] = jnp.where(low, pltpu.roll(keys, HEAD_SIZE, 1), values).astype(jnp.bfloat16)
    loads[2].wait()

    pl.semaphore_wait(barrier, members - 1 + plane)
    for step in range(1, planes):
        @pl.when(plane >= step)
        def _():
            pl.semaphore_signal(
                ready, inc=1, device_id=at(plane - step, member), device_id_type=MESH
            )

    my_rows = pl.ds(pl.multiple_of(member * rows, rows), rows)
    kv_copies, q_copies = [], []
    for turn in range(1, members):
        to = partner(turn)
        copy = pltpu.make_async_remote_copy(
            src_ref=kv_own.at[to],
            dst_ref=kv_buf.at[plane, my_rows],
            send_sem=kv_send.at[turn - 1],
            recv_sem=kv_recv.at[plane],
            device_id=at(plane, to),
            device_id_type=MESH,
        )
        copy.start()
        kv_copies.append(copy)
    pltpu.make_async_copy(kv_own.at[member], kv_buf.at[plane, my_rows], kv_recv.at[plane]).start()
    for tile in range(tiles):
        def query_columns(owner):
            return pl.ds(pl.multiple_of(owner * group_cols + tile * LANES, LANES), LANES)

        for turn in range(1, members):
            to = partner(turn)
            copy = pltpu.make_async_remote_copy(
                src_ref=q_in.at[:, query_columns(to)],
                dst_ref=q_buf.at[tile, my_rows],
                send_sem=q_send.at[tile, turn - 1],
                recv_sem=q_recv.at[tile],
                device_id=at(plane, to),
                device_id_type=MESH,
            )
            copy.start()
            q_copies.append(copy)
        pltpu.make_async_copy(
            q_in.at[:, query_columns(member)], q_buf.at[tile, my_rows], q_recv.at[tile]
        ).start()

    position = plane * slab + lax.broadcasted_iota(jnp.int32, (slab, LANES), 0)
    start = jnp.zeros((slab, LANES), jnp.int32)
    for doc in range(1, bounds_ref.shape[0] - 1):
        bound = bounds_ref[doc]
        start = jnp.where(position >= bound, bound, start)
    doc_start[...] = start

    def fill_bias(slab_start, first, last, causal):
        count = last - first
        for block in range(2):
            here = slice(block * half, (block + 1) * half)
            key = slab_start + first + lax.broadcasted_iota(jnp.int32, (half, count), 1)
            allowed = key >= jnp.tile(doc_start[here], (1, count // LANES))
            if causal:
                query = plane * slab + block * half + lax.broadcasted_iota(jnp.int32, (half, count), 0)
                allowed = allowed & (key <= query)
            bias[here, first:last] = jnp.where(allowed, 0.0, masked_score)

    fill_bias(plane * slab, 0, slab, True)

    pltpu.make_async_copy(kv_buf.at[plane], kv_buf.at[plane], kv_recv.at[plane]).wait()

    def slab_copy(step, first_row):
        piece = kv_buf.at[plane] if first_row == 0 else kv_buf.at[plane, pl.ds(first_row, slab - first_row)]
        return pltpu.make_async_remote_copy(
            src_ref=piece,
            dst_ref=piece,
            send_sem=slab_send.at[step - 1],
            recv_sem=kv_recv.at[plane],
            device_id=at(plane + step, member),
            device_id_type=MESH,
        )

    def each_slab_copy(act):
        for step in range(1, planes):
            to = plane + step
            if reach_start == 0:
                pl.when(to < planes)(lambda: act(slab_copy(step, 0)))
            else:
                early = to < planes // 2
                later = plane > reach_slab if reach_row else plane >= reach_slab
                pl.when((to < planes) & (early | later))(lambda: act(slab_copy(step, 0)))
                if reach_row:
                    part = (to < planes) & (to >= planes // 2) & (plane == reach_slab)
                    pl.when(part)(lambda: act(slab_copy(step, reach_row)))

    pl.when(plane < planes - 1)(lambda: pl.semaphore_wait(ready, planes - 1 - plane))
    each_slab_copy(lambda copy: copy.start())

    def spread(source, first_row):
        low = low_lanes(slab - first_row)
        kv = kv_buf[source, first_row:].astype(jnp.float32)
        swapped = pltpu.roll(kv, HEAD_SIZE, 1)
        key_even[source, first_row:] = jnp.where(low, kv, 0.0).astype(jnp.bfloat16)
        key_odd[source, first_row:] = jnp.where(low, 0.0, swapped).astype(jnp.bfloat16)
        value_even[source, first_row:] = jnp.where(low, swapped, 1.0).astype(jnp.bfloat16)
        value_odd[source, first_row:] = jnp.where(low, 1.0, kv).astype(jnp.bfloat16)

    def attend(tile, block, source, keys, opening, masked):
        here = slice(block * half, (block + 1) * half)
        count = keys.stop - keys.start
        queries = q_buf[tile, here]
        for parity, (key, value) in enumerate(((key_even, value_even), (key_odd, value_odd))):
            scores = lax.dot_general(
                queries, key[source, keys], (((1,), (1,)), ((), ())),
                preferred_element_type=jnp.float32,
            )
            if masked:
                scores = scores + bias[here, keys]
            peak = jnp.max(scores, axis=1, keepdims=True)
            if opening:
                new_top = jnp.broadcast_to(peak, (half, LANES))
            else:
                old_top = top[tile, parity, here]
                new_top = jnp.maximum(old_top, peak)
            weights = jnp.exp2((scores - jnp.tile(new_top, (1, count // LANES))) * exp2_scale)
            mixed = jnp.dot(
                weights.astype(jnp.bfloat16), value[source, keys],
                preferred_element_type=jnp.float32,
            )
            if not opening:
                mixed = mixed + acc[tile, parity, here] * jnp.exp2((old_top - new_top) * exp2_scale)
            top[tile, parity, here] = new_top
            acc[tile, parity, here] = mixed

    spread(plane, 0)
    for tile in range(tiles):
        pltpu.make_async_copy(q_buf.at[tile], q_buf.at[tile], q_recv.at[tile]).wait()
        attend(tile, 0, plane, slice(0, half), True, True)
        attend(tile, 1, plane, slice(0, slab), True, True)

    def fold(tile, source, first_row, masked):
        if masked:
            fill_bias(source * slab, first_row, slab, False)

        @pl.when(tile == 0)
        def _():
            piece = kv_buf.at[source] if first_row == 0 else kv_buf.at[source, pl.ds(first_row, slab - first_row)]
            pltpu.make_async_copy(piece, piece, kv_recv.at[source]).wait()
            spread(source, first_row)

        for block in range(2):
            attend(tile, block, source, slice(first_row, slab), False, masked)

    middle = planes // 2
    clear_slabs = jnp.maximum(plane - middle, 0)
    if reach_start == 0:
        whole_slabs = plane
    else:
        kept = plane - reach_slab - (1 if reach_row else 0)
        whole_slabs = jnp.where(plane < middle, plane, kept)

    def out_copies(tile):
        columns = pl.ds(pl.multiple_of(member * group_cols + tile * LANES, LANES), LANES)
        for turn in range(1, members):
            to = partner(turn)
            yield pltpu.make_async_remote_copy(
                src_ref=o_buf.at[tile, pl.ds(pl.multiple_of(to * rows, rows), rows)],
                dst_ref=out_ref.at[:, columns],
                send_sem=o_send.at[tile, turn - 1],
                recv_sem=o_recv,
                device_id=at(plane, to),
                device_id_type=MESH,
            )

    @pl.loop(0, tiles)
    def _(tile):
        @pl.loop(0, clear_slabs)
        def _(back):
            fold(tile, plane - 1 - back, 0, False)

        @pl.loop(clear_slabs, whole_slabs)
        def _(back):
            fold(tile, plane - 1 - back, 0, True)

        if reach_row:
            pl.when(plane >= middle)(lambda: fold(tile, reach_slab, reach_row, True))

        low = low_lanes(slab)
        even, odd = acc[tile, 0], acc[tile, 1]
        total = pltpu.roll(jnp.where(low, odd, even), HEAD_SIZE, 1)
        o_buf[tile] = (jnp.where(low, even, odd) / total).astype(jnp.bfloat16)
        for copy in out_copies(tile):
            copy.start()
        columns = pl.ds(pl.multiple_of(member * group_cols + tile * LANES, LANES), LANES)
        pltpu.make_async_copy(o_buf.at[tile, my_rows], out_ref.at[:, columns], o_recv).start()

    for copy in kv_copies + q_copies:
        copy.wait_send()
    each_slab_copy(lambda copy: copy.wait_send())
    for tile in range(tiles):
        for copy in out_copies(tile):
            copy.wait_send()
    pltpu.make_async_copy(out_ref, out_ref, o_recv).wait()


def exchange(n_ctx, n_head, reach_start, collective_id, queries, keys, values, doc_bounds):
    rows, query_cols = queries.shape
    members = keys.shape[1] // HEAD_SIZE
    group_cols = query_cols // members
    slab = rows * members
    planes = n_ctx * n_head // members
    tiles = group_cols // LANES
    bf16, f32 = jnp.bfloat16, jnp.float32
    dma = pltpu.SemaphoreType.DMA
    return pl.pallas_call(
        functools.partial(kernel, n_ctx, n_head, members, reach_start),
        out_shape=jax.ShapeDtypeStruct((rows, query_cols), bf16),
        in_specs=[pl.BlockSpec(memory_space=pltpu.SMEM)] + [pl.BlockSpec(memory_space=pl.ANY)] * 3,
        out_specs=pl.BlockSpec(memory_space=pl.ANY),
        scratch_shapes=[
            pltpu.VMEM((rows, query_cols), bf16),
            pltpu.VMEM(keys.shape, bf16),
            pltpu.VMEM(values.shape, bf16),
            pltpu.VMEM((members, rows, LANES), bf16),
            pltpu.VMEM((tiles, slab, LANES), bf16),
            pltpu.VMEM((planes, slab, LANES), bf16),
            pltpu.VMEM((planes, slab, LANES), bf16),
            pltpu.VMEM((planes, slab, LANES), bf16),
            pltpu.VMEM((planes, slab, LANES), bf16),
            pltpu.VMEM((planes, slab, LANES), bf16),
            pltpu.VMEM((slab, LANES), jnp.int32),
            pltpu.VMEM((slab, slab), f32),
            pltpu.VMEM((tiles, 2, slab, LANES), f32),
            pltpu.VMEM((tiles, 2, slab, LANES), f32),
            pltpu.VMEM((tiles, slab, LANES), bf16),
            dma((3,)),
            dma((members - 1,)),
            dma((tiles, members - 1)),
            dma((planes - 1,)),
            dma((tiles, members - 1)),
            dma((planes,)),
            dma((tiles,)),
            dma,
            pltpu.SemaphoreType.REGULAR,
        ],
        compiler_params=pltpu.CompilerParams(collective_id=collective_id, has_side_effects=True),
    )(doc_bounds, queries, keys, values)


def solution(mesh):
    n_ctx, n_head = mesh.shape["ctx"], mesh.shape["head"]

    def on_device(queries, keys, values, doc_bounds):
        tokens = n_ctx * n_head * queries.shape[0]
        reach_start = 3 * tokens // 8

        def near(*arrays):
            return exchange(n_ctx, n_head, reach_start, 0, *arrays)

        def far(*arrays):
            return exchange(n_ctx, n_head, 0, 1, *arrays)

        return lax.cond(doc_bounds[-2] >= reach_start, near, far, queries, keys, values, doc_bounds)

    return jax.shard_map(
        on_device,
        mesh=mesh,
        in_specs=(P(("ctx", "head"), None),) * 3 + (P(),),
        out_specs=P(("ctx", "head"), None),
        check_vma=False,
    )
```

```python
import functools
import math

import jax
import jax.numpy as jnp
from jax import lax
from jax.experimental import pallas as pl
from jax.experimental.pallas import tpu as pltpu
from jax.sharding import PartitionSpec as P

HEAD_SIZE = 64
LANES = 128
MESH = pl.DeviceIdType.MESH

masked_score = -1e30
exp2_scale = math.log2(math.e) / math.sqrt(HEAD_SIZE)


def kernel(
    n_ctx, n_head, members, reach_piece,
    bounds_ref, q_hbm, k_hbm, v_hbm, out_ref,
    q_in, k_in, v_in, kv_own, q_buf, kv_buf, key_even, key_odd, value_even, value_odd,
    doc_start, bias, piece_bias, top, acc, o_buf,
    in_sem, kv_send, q_send, piece_send, o_send, kv_recv, piece_recv, q_recv, o_recv, ready,
):
    rows = q_in.shape[0]
    group_cols = q_in.shape[1] // members
    tiles = group_cols // LANES
    slab = rows * members
    half = slab // 2
    span = members // n_head
    planes = n_ctx // span
    my_ctx, my_head = lax.axis_index("ctx"), lax.axis_index("head")
    plane = my_ctx // span
    member = lax.rem(my_ctx, span) * n_head + my_head
    middle = planes // 2

    def at(plane_index, member_index):
        return (plane_index * span + member_index // n_head, lax.rem(member_index, n_head))

    def partner(turn):
        return lax.rem(member + turn, members)

    loads = [
        pltpu.make_async_copy(k_hbm, k_in, in_sem.at[0]),
        pltpu.make_async_copy(v_hbm, v_in, in_sem.at[1]),
        pltpu.make_async_copy(q_hbm, q_in, in_sem.at[2]),
    ]
    for load in loads:
        load.start()

    barrier = pltpu.get_barrier_semaphore()
    for turn in range(1, members):
        pl.semaphore_signal(barrier, inc=1, device_id=at(plane, partner(turn)), device_id_type=MESH)
    for step in range(1, planes):
        @pl.when(plane + step < planes)
        def _():
            pl.semaphore_signal(
                barrier, inc=1, device_id=at(plane + step, member), device_id_type=MESH
            )

    def low_lanes(count):
        return lax.broadcasted_iota(jnp.int32, (count, LANES), 1) < HEAD_SIZE

    loads[0].wait()
    loads[1].wait()
    low = low_lanes(rows)
    for pair in range(members // 2):
        columns = slice(pair * LANES, (pair + 1) * LANES)
        keys = k_in[:, columns].astype(jnp.float32)
        values = v_in[:, columns].astype(jnp.float32)
        kv_own[2 * pair] = jnp.where(low, keys, pltpu.roll(values, HEAD_SIZE, 1)).astype(jnp.bfloat16)
        kv_own[2 * pair + 1] = jnp.where(low, pltpu.roll(keys, HEAD_SIZE, 1), values).astype(jnp.bfloat16)
    loads[2].wait()

    pl.semaphore_wait(barrier, members - 1 + plane)
    for step in range(1, planes):
        @pl.when(plane >= step)
        def _():
            pl.semaphore_signal(
                ready, inc=1, device_id=at(plane - step, member), device_id_type=MESH
            )

    my_rows = pl.ds(pl.multiple_of(member * rows, rows), rows)
    my_piece = 2 * plane + member // (members // 2)
    piece_rows = pl.ds(pl.multiple_of(lax.rem(member, members // 2) * rows, rows), rows)
    my_slab = kv_buf.at[pl.ds(2 * plane, 2)]
    kv_copies, q_copies = [], []
    for turn in range(1, members):
        to = partner(turn)
        copy = pltpu.make_async_remote_copy(
            src_ref=kv_own.at[to],
            dst_ref=kv_buf.at[my_piece, piece_rows],
            send_sem=kv_send.at[turn - 1],
            recv_sem=kv_recv,
            device_id=at(plane, to),
            device_id_type=MESH,
        )
        copy.start()
        kv_copies.append(copy)
    pltpu.make_async_copy(kv_own.at[member], kv_buf.at[my_piece, piece_rows], kv_recv).start()
    for tile in range(tiles):
        def query_columns(owner):
            return pl.ds(pl.multiple_of(owner * group_cols + tile * LANES, LANES), LANES)

        for turn in range(1, members):
            to = partner(turn)
            copy = pltpu.make_async_remote_copy(
                src_ref=q_in.at[:, query_columns(to)],
                dst_ref=q_buf.at[tile, my_rows],
                send_sem=q_send.at[tile, turn - 1],
                recv_sem=q_recv.at[tile],
                device_id=at(plane, to),
                device_id_type=MESH,
            )
            copy.start()
            q_copies.append(copy)
        pltpu.make_async_copy(
            q_in.at[:, query_columns(member)], q_buf.at[tile, my_rows], q_recv.at[tile]
        ).start()

    position = plane * slab + lax.broadcasted_iota(jnp.int32, (slab, LANES), 0)
    start = jnp.zeros((slab, LANES), jnp.int32)
    for doc in range(1, bounds_ref.shape[0] - 1):
        bound = bounds_ref[doc]
        start = jnp.where(position >= bound, bound, start)
    doc_start[...] = start

    def fill_bias(into, first_key, causal):
        count = into.shape[1]
        for block in range(2):
            here = slice(block * half, (block + 1) * half)
            key = first_key + lax.broadcasted_iota(jnp.int32, (half, count), 1)
            allowed = key >= jnp.tile(doc_start[here], (1, count // LANES))
            if causal:
                query = plane * slab + block * half + lax.broadcasted_iota(jnp.int32, (half, count), 0)
                allowed = allowed & (key <= query)
            into[here] = jnp.where(allowed, 0.0, masked_score)

    fill_bias(bias, plane * slab, True)

    pltpu.make_async_copy(my_slab, my_slab, kv_recv).wait()

    def each_piece_copy(act):
        for step in range(planes - 1, 0, -1):
            to = plane + step
            for part in range(2):
                piece = 2 * plane + part

                @pl.when((to < planes) & ((to < middle) | (piece >= reach_piece)))
                def _():
                    act(pltpu.make_async_remote_copy(
                        src_ref=kv_buf.at[piece],
                        dst_ref=kv_buf.at[piece],
                        send_sem=piece_send.at[step - 1, part],
                        recv_sem=piece_recv.at[piece],
                        device_id=at(to, member),
                        device_id_type=MESH,
                    ))

    pl.when(plane < planes - 1)(lambda: pl.semaphore_wait(ready, planes - 1 - plane))
    each_piece_copy(lambda copy: copy.start())

    def spread(piece, to):
        low = low_lanes(half)
        kv = kv_buf[piece].astype(jnp.float32)
        swapped = pltpu.roll(kv, HEAD_SIZE, 1)
        key_even[to] = jnp.where(low, kv, 0.0).astype(jnp.bfloat16)
        key_odd[to] = jnp.where(low, 0.0, swapped).astype(jnp.bfloat16)
        value_even[to] = jnp.where(low, swapped, 1.0).astype(jnp.bfloat16)
        value_odd[to] = jnp.where(low, 1.0, kv).astype(jnp.bfloat16)

    def attend(tile, block, count, added, opening):
        here = slice(block * half, (block + 1) * half)
        queries = q_buf[tile, here]
        for parity, (key, value) in enumerate(((key_even, value_even), (key_odd, value_odd))):
            scores = lax.dot_general(
                queries, key[:count], (((1,), (1,)), ((), ())), preferred_element_type=jnp.float32
            ) + added[here, :count]
            peak = jnp.max(scores, axis=1, keepdims=True)
            if opening:
                new_top = jnp.broadcast_to(peak, (half, LANES))
            else:
                old_top = top[tile, parity, here]
                new_top = jnp.maximum(old_top, peak)
            weights = jnp.exp2((scores - jnp.tile(new_top, (1, count // LANES))) * exp2_scale)
            mixed = jnp.dot(
                weights.astype(jnp.bfloat16), value[:count], preferred_element_type=jnp.float32
            )
            if not opening:
                mixed = mixed + acc[tile, parity, here] * jnp.exp2((old_top - new_top) * exp2_scale)
            top[tile, parity, here] = new_top
            acc[tile, parity, here] = mixed

    spread(2 * plane, slice(0, half))
    spread(2 * plane + 1, slice(half, slab))
    for tile in range(tiles):
        pltpu.make_async_copy(q_buf.at[tile], q_buf.at[tile], q_recv.at[tile]).wait()
        attend(tile, 0, half, bias, True)
        attend(tile, 1, slab, bias, True)

    def prepare(piece):
        fill_bias(piece_bias, piece * half, False)
        pltpu.make_async_copy(kv_buf.at[piece], kv_buf.at[piece], piece_recv.at[piece]).wait()
        spread(piece, slice(0, half))

    def fold(tile):
        for block in range(2):
            attend(tile, block, half, piece_bias, False)

    first_piece = jnp.where(plane < middle, 0, reach_piece)
    last_piece = 2 * plane - 1
    behind = last_piece >= first_piece

    @pl.loop(first_piece, jnp.maximum(last_piece, first_piece))
    def _(piece):
        prepare(piece)
        for tile in range(tiles):
            fold(tile)

    pl.when(behind)(lambda: prepare(last_piece))

    def out_copies(tile):
        columns = pl.ds(pl.multiple_of(member * group_cols + tile * LANES, LANES), LANES)
        for turn in range(1, members):
            to = partner(turn)
            yield pltpu.make_async_remote_copy(
                src_ref=o_buf.at[tile, pl.ds(pl.multiple_of(to * rows, rows), rows)],
                dst_ref=out_ref.at[:, columns],
                send_sem=o_send.at[tile, turn - 1],
                recv_sem=o_recv,
                device_id=at(plane, to),
                device_id_type=MESH,
            )

    @pl.loop(0, tiles)
    def _(tile):
        pl.when(behind)(lambda: fold(tile))
        low = low_lanes(slab)
        even, odd = acc[tile, 0], acc[tile, 1]
        total = pltpu.roll(jnp.where(low, odd, even), HEAD_SIZE, 1)
        o_buf[tile] = (jnp.where(low, even, odd) / total).astype(jnp.bfloat16)
        for copy in out_copies(tile):
            copy.start()
        columns = pl.ds(pl.multiple_of(member * group_cols + tile * LANES, LANES), LANES)
        pltpu.make_async_copy(o_buf.at[tile, my_rows], out_ref.at[:, columns], o_recv).start()

    for copy in kv_copies + q_copies:
        copy.wait_send()
    each_piece_copy(lambda copy: copy.wait_send())
    for tile in range(tiles):
        for copy in out_copies(tile):
            copy.wait_send()
    pltpu.make_async_copy(out_ref, out_ref, o_recv).wait()


def reach_of(planes):
    return 3 * planes // 4


def exchange(n_ctx, n_head, near, collective_id, queries, keys, values, doc_bounds):
    rows, query_cols = queries.shape
    members = keys.shape[1] // HEAD_SIZE
    group_cols = query_cols // members
    slab = rows * members
    planes = n_ctx * n_head // members
    reach_piece = reach_of(planes) if near else 0
    half = slab // 2
    tiles = group_cols // LANES
    bf16, f32 = jnp.bfloat16, jnp.float32
    dma = pltpu.SemaphoreType.DMA
    return pl.pallas_call(
        functools.partial(kernel, n_ctx, n_head, members, reach_piece),
        out_shape=jax.ShapeDtypeStruct((rows, query_cols), bf16),
        in_specs=[pl.BlockSpec(memory_space=pltpu.SMEM)] + [pl.BlockSpec(memory_space=pl.ANY)] * 3,
        out_specs=pl.BlockSpec(memory_space=pl.ANY),
        scratch_shapes=[
            pltpu.VMEM((rows, query_cols), bf16),
            pltpu.VMEM(keys.shape, bf16),
            pltpu.VMEM(values.shape, bf16),
            pltpu.VMEM((members, rows, LANES), bf16),
            pltpu.VMEM((tiles, slab, LANES), bf16),
            pltpu.VMEM((2 * planes, half, LANES), bf16),
            pltpu.VMEM((slab, LANES), bf16),
            pltpu.VMEM((slab, LANES), bf16),
            pltpu.VMEM((slab, LANES), bf16),
            pltpu.VMEM((slab, LANES), bf16),
            pltpu.VMEM((slab, LANES), jnp.int32),
            pltpu.VMEM((slab, slab), f32),
            pltpu.VMEM((slab, half), f32),
            pltpu.VMEM((tiles, 2, slab, LANES), f32),
            pltpu.VMEM((tiles, 2, slab, LANES), f32),
            pltpu.VMEM((tiles, slab, LANES), bf16),
            dma((3,)),
            dma((members - 1,)),
            dma((tiles, members - 1)),
            dma((planes - 1, 2)),
            dma((tiles, members - 1)),
            dma,
            dma((2 * planes,)),
            dma((tiles,)),
            dma,
            pltpu.SemaphoreType.REGULAR,
        ],
        compiler_params=pltpu.CompilerParams(collective_id=collective_id, has_side_effects=True),
    )(doc_bounds, queries, keys, values)


def solution(mesh):
    n_ctx, n_head = mesh.shape["ctx"], mesh.shape["head"]

    def on_device(queries, keys, values, doc_bounds):
        slab = queries.shape[0] * (keys.shape[1] // HEAD_SIZE)
        planes = n_ctx * n_head * queries.shape[0] // slab
        reach_start = reach_of(planes) * (slab // 2)

        def near(*arrays):
            return exchange(n_ctx, n_head, True, 0, *arrays)

        def far(*arrays):
            return exchange(n_ctx, n_head, False, 1, *arrays)

        return lax.cond(doc_bounds[-2] >= reach_start, near, far, queries, keys, values, doc_bounds)

    return jax.shard_map(
        on_device,
        mesh=mesh,
        in_specs=(P(("ctx", "head"), None),) * 3 + (P(),),
        out_specs=P(("ctx", "head"), None),
        check_vma=False,
    )
```

```python
import functools
import math

import jax
import jax.numpy as jnp
from jax import lax
from jax.experimental import pallas as pl
from jax.experimental.pallas import tpu as pltpu
from jax.sharding import PartitionSpec as P

HEAD_SIZE = 64
LANES = 128
MESH = pl.DeviceIdType.MESH

masked_score = -1e30
exp2_scale = math.log2(math.e) / math.sqrt(HEAD_SIZE)


def kernel(
    n_ctx, n_head, members, reach_piece,
    bounds_hbm, q_hbm, k_hbm, v_hbm, out_ref,
    bounds_ref, q_in, k_in, v_in, kv_own, q_buf, kv_buf, key_even, key_odd, value_even, value_odd,
    doc_start, bias, piece_bias, top, acc, o_buf,
    in_sem, kv_send, q_send, piece_send, o_send, kv_recv, piece_recv, q_recv, o_recv, ready,
):
    rows = q_in.shape[0]
    group_cols = q_in.shape[1] // members
    tiles = group_cols // LANES
    slab = rows * members
    half = slab // 2
    span = members // n_head
    planes = n_ctx // span
    my_ctx, my_head = lax.axis_index("ctx"), lax.axis_index("head")
    plane = my_ctx // span
    member = lax.rem(my_ctx, span) * n_head + my_head
    middle = planes // 2

    def at(plane_index, member_index):
        return (plane_index * span + member_index // n_head, lax.rem(member_index, n_head))

    def partner(turn):
        return lax.rem(member + turn, members)

    barrier = pltpu.get_barrier_semaphore()
    for turn in range(1, members):
        pl.semaphore_signal(barrier, inc=1, device_id=at(plane, partner(turn)), device_id_type=MESH)
    for step in range(1, planes):
        @pl.when(plane + step < planes)
        def _():
            pl.semaphore_signal(
                barrier, inc=1, device_id=at(plane + step, member), device_id_type=MESH
            )

    loads = [
        pltpu.make_async_copy(k_hbm, k_in, in_sem.at[0]),
        pltpu.make_async_copy(v_hbm, v_in, in_sem.at[1]),
        pltpu.make_async_copy(q_hbm, q_in, in_sem.at[2]),
        pltpu.make_async_copy(bounds_hbm, bounds_ref, in_sem.at[3]),
    ]
    for load in loads:
        load.start()

    def low_lanes(count):
        return lax.broadcasted_iota(jnp.int32, (count, LANES), 1) < HEAD_SIZE

    loads[0].wait()
    loads[1].wait()
    low = low_lanes(rows)
    for pair in range(members // 2):
        columns = slice(pair * LANES, (pair + 1) * LANES)
        keys = k_in[:, columns].astype(jnp.float32)
        values = v_in[:, columns].astype(jnp.float32)
        kv_own[2 * pair] = jnp.where(low, keys, pltpu.roll(values, HEAD_SIZE, 1)).astype(jnp.bfloat16)
        kv_own[2 * pair + 1] = jnp.where(low, pltpu.roll(keys, HEAD_SIZE, 1), values).astype(jnp.bfloat16)
    loads[2].wait()

    pl.semaphore_wait(barrier, members - 1 + plane)
    for step in range(1, planes):
        @pl.when(plane >= step)
        def _():
            pl.semaphore_signal(
                ready, inc=1, device_id=at(plane - step, member), device_id_type=MESH
            )

    my_rows = pl.ds(pl.multiple_of(member * rows, rows), rows)
    my_piece = 2 * plane + member // (members // 2)
    piece_rows = pl.ds(pl.multiple_of(lax.rem(member, members // 2) * rows, rows), rows)
    my_slab = kv_buf.at[pl.ds(2 * plane, 2)]
    kv_copies, q_copies = [], []
    for turn in range(1, members):
        to = partner(turn)
        copy = pltpu.make_async_remote_copy(
            src_ref=kv_own.at[to],
            dst_ref=kv_buf.at[my_piece, piece_rows],
            send_sem=kv_send.at[turn - 1],
            recv_sem=kv_recv,
            device_id=at(plane, to),
            device_id_type=MESH,
        )
        copy.start()
        kv_copies.append(copy)
    pltpu.make_async_copy(kv_own.at[member], kv_buf.at[my_piece, piece_rows], kv_recv).start()
    for tile in range(tiles):
        def query_columns(owner):
            return pl.ds(pl.multiple_of(owner * group_cols + tile * LANES, LANES), LANES)

        for turn in range(1, members):
            to = partner(turn)
            copy = pltpu.make_async_remote_copy(
                src_ref=q_in.at[:, query_columns(to)],
                dst_ref=q_buf.at[tile, my_rows],
                send_sem=q_send.at[tile, turn - 1],
                recv_sem=q_recv.at[tile],
                device_id=at(plane, to),
                device_id_type=MESH,
            )
            copy.start()
            q_copies.append(copy)
        pltpu.make_async_copy(
            q_in.at[:, query_columns(member)], q_buf.at[tile, my_rows], q_recv.at[tile]
        ).start()

    loads[3].wait()
    position = plane * slab + lax.broadcasted_iota(jnp.int32, (slab, LANES), 0)
    start = jnp.zeros((slab, LANES), jnp.int32)
    for doc in range(1, bounds_ref.shape[0] - 1):
        bound = bounds_ref[doc]
        start = jnp.where(position >= bound, bound, start)
    doc_start[...] = start

    def fill_bias(into, first_key, causal):
        count = into.shape[1]
        for block in range(2):
            here = slice(block * half, (block + 1) * half)
            key = first_key + lax.broadcasted_iota(jnp.int32, (half, count), 1)
            allowed = key >= jnp.tile(doc_start[here], (1, count // LANES))
            if causal:
                query = plane * slab + block * half + lax.broadcasted_iota(jnp.int32, (half, count), 0)
                allowed = allowed & (key <= query)
            into[here] = jnp.where(allowed, 0.0, masked_score)

    fill_bias(bias, plane * slab, True)

    pltpu.make_async_copy(my_slab, my_slab, kv_recv).wait()

    def each_piece_copy(act):
        for step in range(planes - 1, 0, -1):
            to = plane + step
            for part in range(2):
                piece = 2 * plane + part

                @pl.when((to < planes) & ((to < middle) | (piece >= reach_piece)))
                def _():
                    act(pltpu.make_async_remote_copy(
                        src_ref=kv_buf.at[piece],
                        dst_ref=kv_buf.at[piece],
                        send_sem=piece_send.at[step - 1, part],
                        recv_sem=piece_recv.at[piece],
                        device_id=at(to, member),
                        device_id_type=MESH,
                    ))

    pl.when(plane < planes - 1)(lambda: pl.semaphore_wait(ready, planes - 1 - plane))
    each_piece_copy(lambda copy: copy.start())

    def spread(piece, to):
        low = low_lanes(half)
        kv = kv_buf[piece].astype(jnp.float32)
        swapped = pltpu.roll(kv, HEAD_SIZE, 1)
        key_even[to] = jnp.where(low, kv, 0.0).astype(jnp.bfloat16)
        key_odd[to] = jnp.where(low, 0.0, swapped).astype(jnp.bfloat16)
        value_even[to] = jnp.where(low, swapped, 1.0).astype(jnp.bfloat16)
        value_odd[to] = jnp.where(low, 1.0, kv).astype(jnp.bfloat16)

    def attend(tile, block, count, added, opening):
        here = slice(block * half, (block + 1) * half)
        queries = q_buf[tile, here]
        for parity, (key, value) in enumerate(((key_even, value_even), (key_odd, value_odd))):
            scores = lax.dot_general(
                queries, key[:count], (((1,), (1,)), ((), ())), preferred_element_type=jnp.float32
            ) + added[here, :count]
            peak = jnp.max(scores, axis=1, keepdims=True)
            if opening:
                new_top = jnp.broadcast_to(peak, (half, LANES))
            else:
                old_top = top[tile, parity, here]
                new_top = jnp.maximum(old_top, peak)
            weights = jnp.exp2((scores - jnp.tile(new_top, (1, count // LANES))) * exp2_scale)
            mixed = jnp.dot(
                weights.astype(jnp.bfloat16), value[:count], preferred_element_type=jnp.float32
            )
            if not opening:
                mixed = mixed + acc[tile, parity, here] * jnp.exp2((old_top - new_top) * exp2_scale)
            top[tile, parity, here] = new_top
            acc[tile, parity, here] = mixed

    spread(2 * plane, slice(0, half))
    spread(2 * plane + 1, slice(half, slab))
    for tile in range(tiles):
        pltpu.make_async_copy(q_buf.at[tile], q_buf.at[tile], q_recv.at[tile]).wait()
        attend(tile, 0, half, bias, True)
        attend(tile, 1, slab, bias, True)

    def prepare(piece):
        fill_bias(piece_bias, piece * half, False)
        pltpu.make_async_copy(kv_buf.at[piece], kv_buf.at[piece], piece_recv.at[piece]).wait()
        spread(piece, slice(0, half))

    def fold(tile):
        for block in range(2):
            attend(tile, block, half, piece_bias, False)

    first_piece = jnp.where(plane < middle, 0, reach_piece)
    last_piece = 2 * plane - 1
    behind = last_piece >= first_piece

    @pl.loop(first_piece, jnp.maximum(last_piece, first_piece))
    def _(piece):
        prepare(piece)
        for tile in range(tiles):
            fold(tile)

    pl.when(behind)(lambda: prepare(last_piece))

    def out_copies(tile):
        columns = pl.ds(pl.multiple_of(member * group_cols + tile * LANES, LANES), LANES)
        for turn in range(1, members):
            to = partner(turn)
            yield pltpu.make_async_remote_copy(
                src_ref=o_buf.at[tile, pl.ds(pl.multiple_of(to * rows, rows), rows)],
                dst_ref=out_ref.at[:, columns],
                send_sem=o_send.at[tile, turn - 1],
                recv_sem=o_recv,
                device_id=at(plane, to),
                device_id_type=MESH,
            )

    @pl.loop(0, tiles)
    def _(tile):
        pl.when(behind)(lambda: fold(tile))
        low = low_lanes(slab)
        even, odd = acc[tile, 0], acc[tile, 1]
        total = pltpu.roll(jnp.where(low, odd, even), HEAD_SIZE, 1)
        o_buf[tile] = (jnp.where(low, even, odd) / total).astype(jnp.bfloat16)
        for copy in out_copies(tile):
            copy.start()
        columns = pl.ds(pl.multiple_of(member * group_cols + tile * LANES, LANES), LANES)
        pltpu.make_async_copy(o_buf.at[tile, my_rows], out_ref.at[:, columns], o_recv).start()

    for copy in kv_copies + q_copies:
        copy.wait_send()
    each_piece_copy(lambda copy: copy.wait_send())
    for tile in range(tiles):
        for copy in out_copies(tile):
            copy.wait_send()
    pltpu.make_async_copy(out_ref, out_ref, o_recv).wait()


def reach_of(planes):
    return 3 * planes // 4


def exchange(n_ctx, n_head, near, collective_id, queries, keys, values, doc_bounds):
    rows, query_cols = queries.shape
    members = keys.shape[1] // HEAD_SIZE
    group_cols = query_cols // members
    slab = rows * members
    planes = n_ctx * n_head // members
    reach_piece = reach_of(planes) if near else 0
    half = slab // 2
    tiles = group_cols // LANES
    bf16, f32 = jnp.bfloat16, jnp.float32
    dma = pltpu.SemaphoreType.DMA
    return pl.pallas_call(
        functools.partial(kernel, n_ctx, n_head, members, reach_piece),
        out_shape=jax.ShapeDtypeStruct((rows, query_cols), bf16),
        in_specs=[pl.BlockSpec(memory_space=pltpu.HBM)] * 4,
        out_specs=pl.BlockSpec(memory_space=pl.ANY),
        scratch_shapes=[
            pltpu.SMEM(doc_bounds.shape, jnp.int32),
            pltpu.VMEM((rows, query_cols), bf16),
            pltpu.VMEM(keys.shape, bf16),
            pltpu.VMEM(values.shape, bf16),
            pltpu.VMEM((members, rows, LANES), bf16),
            pltpu.VMEM((tiles, slab, LANES), bf16),
            pltpu.VMEM((2 * planes, half, LANES), bf16),
            pltpu.VMEM((slab, LANES), bf16),
            pltpu.VMEM((slab, LANES), bf16),
            pltpu.VMEM((slab, LANES), bf16),
            pltpu.VMEM((slab, LANES), bf16),
            pltpu.VMEM((slab, LANES), jnp.int32),
            pltpu.VMEM((slab, slab), f32),
            pltpu.VMEM((slab, half), f32),
            pltpu.VMEM((tiles, 2, slab, LANES), f32),
            pltpu.VMEM((tiles, 2, slab, LANES), f32),
            pltpu.VMEM((tiles, slab, LANES), bf16),
            dma((4,)),
            dma((members - 1,)),
            dma((tiles, members - 1)),
            dma((planes - 1, 2)),
            dma((tiles, members - 1)),
            dma,
            dma((2 * planes,)),
            dma((tiles,)),
            dma,
            pltpu.SemaphoreType.REGULAR,
        ],
        compiler_params=pltpu.CompilerParams(collective_id=collective_id, has_side_effects=True),
    )(doc_bounds, queries, keys, values)


def solution(mesh):
    n_ctx, n_head = mesh.shape["ctx"], mesh.shape["head"]

    def on_device(queries, keys, values, doc_bounds):
        slab = queries.shape[0] * (keys.shape[1] // HEAD_SIZE)
        planes = n_ctx * n_head * queries.shape[0] // slab
        reach_start = reach_of(planes) * (slab // 2)

        def near(*arrays):
            return exchange(n_ctx, n_head, True, 0, *arrays)

        def far(*arrays):
            return exchange(n_ctx, n_head, False, 1, *arrays)

        return lax.cond(doc_bounds[-2] >= reach_start, near, far, queries, keys, values, doc_bounds)

    return jax.shard_map(
        on_device,
        mesh=mesh,
        in_specs=(P(("ctx", "head"), None),) * 3 + (P(),),
        out_specs=P(("ctx", "head"), None),
        check_vma=False,
    )
```
